32 devices in a mesh: dp: 8 (over z, y), feat: 4 (over x, core).
Axes of the slice: x: 2, y: 2, z: 4, core: 2. Of those that a mesh axis runs over, the one named last changes fastest.
Arguments:
- observations: bfloat16 [1024, 128, 128], P('dp', 'feat'), may hold values from -1.5 to 1.5
- labels: int32 [1024, 128], P('dp'), may hold values 0 or 1
- tile_live: int32 [1024], P('dp'), may hold values from 1 to 128
- tile_group: int32 [1024], P('dp'), may hold values from 0 to 127, as said below
- position: float32 [128, 2048], P('dp', 'feat'), may hold values from -2.4 to 2.4
- momentum: float32 [128, 2048], P('dp', 'feat'), may hold values from -6 to 6
- gradient: float32 [128, 2048], P('dp', 'feat'), may hold values from -18 to 18
- prior_mean: float32 [2048], P('feat'), may hold values from -1.8 to 1.8
- prior_prec: float32 [128], P('feat'), may hold values from 0.25 to 4
- inv_mass: float32 [128], P('feat'), may hold values from 0.5 to 2
Outputs:
- new_position: float32 [128, 2048], P('dp', 'feat')
- new_momentum: float32 [128, 2048], P('dp', 'feat')
- new_gradient: float32 [128, 2048], P('dp', 'feat')
- energy: float32 [128, 16], P('dp')
The draws below stay inside these ranges and needn't reach their ends.
Inputs may be any that keep to these rules, and one draw needn't show every extreme that they name: `tile_group`: group g belongs to owner g // 16. Among the 128 tiles of one device at most 32 have groups of any one owner, and one owner has exactly 32 tiles from every device. `tile_live`: the live slots of a tile come first.
All inputs are finite; a program needn't handle non-finite values. No bound on the sum of `labels` on one device may be relied on, other than what follows from the above.
Results may differ from the reference program's by a relative error of at most 0.0041.
Values may be sent and summed in bfloat16 or wider, within the bound.
A program may use at most 64 MiB of HBM per device.

```python
import math
import jax
import jax.numpy as jnp
from jax import lax

F = 128
ROWS = 128
TILE_DEV = 128
GRP_DEV = 16
CHAINS = 16
NTILES = 1024
GROUPS = 128


def draw_tile_group(key, part):
    owners = GROUPS // GRP_DEV
    block_total = NTILES // TILE_DEV
    slot_count = max(2, 2 * TILE_DEV // owners)
    hot_owner = jax.random.randint(jax.random.fold_in(key, 11), (), 0, owners)
    spare_count = (owners - 1) * slot_count

    def one_block(block_index):
        block_key = jax.random.fold_in(jax.random.fold_in(key, 12), block_index)
        pick_key, order_key, local_key = jax.random.split(block_key, 3)
        candidate = jnp.arange(spare_count, dtype=jnp.int32) // slot_count
        candidate = candidate + (candidate >= hot_owner).astype(jnp.int32)
        chosen = jax.random.permutation(pick_key, candidate)[:TILE_DEV - slot_count]
        target = jnp.concatenate([jnp.full((slot_count,), hot_owner, jnp.int32), chosen.astype(jnp.int32)])
        target = jax.random.permutation(order_key, target)
        local_group = jax.random.randint(local_key, (TILE_DEV,), 0, GRP_DEV)
        return (target * GRP_DEV + local_group).astype(jnp.int32)
    return jax.vmap(one_block)(jnp.arange(block_total, dtype=jnp.int32)).reshape(NTILES).astype(jnp.int32)


def set_ends(drawn, rng, smallest, high):
    shape = drawn.shape
    index_at = [jax.random.randint(jax.random.fold_in(rng, axis), (), 0, shape[axis]) for axis in range(len(shape))]
    drawn = drawn.at[tuple(index_at)].set(smallest)
    longest = shape.index(max(shape))
    index_at[longest] = (index_at[longest] + 1) % shape[longest]
    return drawn.at[tuple(index_at)].set(high)


def block_levels(rng, dims, pieces, low, high):
    loudness = 1.0
    for dim, blocks in pieces:
        draws = jax.random.uniform(jax.random.fold_in(jax.random.fold_in(rng, 6), dim), (blocks,), jnp.float32, low / len(pieces), high / len(pieces))
        loudness = loudness * jnp.repeat(jnp.exp(draws), dims[dim] // blocks).reshape((-1,) + (1,) * (len(dims) - 1 - dim))
    return loudness


def noise(own_key, extent, width, most, pieces=(), kind=jnp.bfloat16):
    factor_of = block_levels(own_key, extent, pieces, -0.22, 0.18) if pieces else 1.0
    result = jax.random.normal(own_key, extent, jnp.float32) * width * factor_of
    return jnp.minimum(jnp.maximum(result, -most), most).astype(kind)


def setup_inputs(seed: int = 0) -> dict:
    arg_keys = jax.random.split(jax.random.key(seed), 11)
    observations = noise(arg_keys[0], (NTILES, F, ROWS), 0.25, 1.5, ((0, 8), (1, 4)))
    labels = set_ends((jax.random.randint(arg_keys[1], (NTILES, ROWS), 0, 2) < 1).astype(jnp.int32), jax.random.fold_in(arg_keys[1], 1), 0, 1)
    tile_live = set_ends(jax.random.randint(arg_keys[2], (NTILES,), 1, ROWS + 1), jax.random.fold_in(arg_keys[2], 1), 1, ROWS).astype(jnp.int32)
    tile_group = draw_tile_group(jax.random.fold_in(arg_keys[10], 71), 0)
    position = noise(arg_keys[4], (GROUPS, F * CHAINS), 0.4, 2.4, ((0, 8), (1, 4)), jnp.float32)
    momentum = noise(arg_keys[5], (GROUPS, F * CHAINS), 1.0, 6.0, ((0, 8), (1, 4)), jnp.float32)
    gradient = noise(arg_keys[6], (GROUPS, F * CHAINS), 3.0, 18.0, ((0, 8), (1, 4)), jnp.float32)
    prior_mean = noise(arg_keys[7], (F * CHAINS,), 0.3, 1.8, ((0, 4),), jnp.float32)
    prior_prec = jnp.clip(jnp.exp(math.log(4.0) - 2.7725887 * jax.random.uniform(arg_keys[8], (F,), jnp.float32) ** block_levels(arg_keys[8], (F,), ((0, 4),), -0.2, 0.2)), 0.25, 4.0)
    inv_mass = jnp.clip(jnp.exp(math.log(2.0) - 1.3862944 * jax.random.uniform(arg_keys[9], (F,), jnp.float32) ** block_levels(arg_keys[9], (F,), ((0, 4),), -0.2, 0.2)), 0.5, 2.0)
    return {"observations": observations, "labels": labels, "tile_live": tile_live, "tile_group": tile_group, "position": position, "momentum": momentum, "gradient": gradient, "prior_mean": prior_mean, "prior_prec": prior_prec, "inv_mass": inv_mass}


step_size = 0.1


def tile_terms(blocks, observations, labels, tile_live):
    logits = jnp.einsum("tfc,tfr->tcr", blocks.astype(jnp.float32), observations.astype(jnp.float32), precision=lax.Precision.HIGHEST)
    live_rows = (jnp.arange(observations.shape[2], dtype=jnp.int32)[None, :] < tile_live[:, None])[:, None, :]
    targets = labels.astype(jnp.float32)[:, None, :]
    residual = jnp.where(live_rows, jax.nn.sigmoid(logits) - targets, 0.0).astype(jnp.bfloat16)
    neg_loglik = jnp.sum(jnp.where(live_rows, jax.nn.softplus(logits) - targets * logits, 0.0), axis=2)
    partial_value = jnp.einsum("tfr,tcr->tfc", observations.astype(jnp.float32), residual.astype(jnp.float32), precision=lax.Precision.HIGHEST)
    return partial_value.reshape(partial_value.shape[0], -1), neg_loglik


def reference(observations, labels, tile_live, tile_group, position, momentum, gradient, prior_mean, prior_prec, inv_mass):
    prior_full = jnp.repeat(prior_prec, CHAINS)
    mass_full = jnp.repeat(inv_mass, CHAINS)
    half_momentum = momentum - 0.5 * step_size * gradient
    moved_position = position + step_size * mass_full * half_momentum
    rounded = moved_position.astype(jnp.bfloat16)
    block_total = NTILES // TILE_DEV

    def one_block(running, block_items):
        tile_obs, tile_labels, live_count, groups = block_items
        blocks = rounded[groups].reshape(groups.shape[0], F, CHAINS)
        partial_value, neg_loglik = tile_terms(blocks, tile_obs, tile_labels, live_count)
        return running, (partial_value, neg_loglik)

    block_items = (observations.reshape(block_total, TILE_DEV, F, ROWS), labels.reshape(block_total, TILE_DEV, ROWS), tile_live.reshape(block_total, TILE_DEV), tile_group.reshape(block_total, TILE_DEV))
    running, outputs = lax.scan(one_block, jnp.zeros((), jnp.float32), block_items)
    partials, losses = outputs
    likelihood_grad = jax.ops.segment_sum(partials.reshape(NTILES, F * CHAINS), tile_group, num_segments=GROUPS)
    group_loglik = jax.ops.segment_sum(losses.reshape(NTILES, CHAINS), tile_group, num_segments=GROUPS)
    offset = moved_position - prior_mean
    new_gradient = likelihood_grad + prior_full * offset
    new_momentum = half_momentum - 0.5 * step_size * new_gradient
    quadratic = 0.5 * (prior_full * offset * offset + mass_full * new_momentum * new_momentum)
    energy = group_loglik + jnp.sum(quadratic.reshape(GROUPS, F, CHAINS), axis=1)
    return moved_position, new_momentum, new_gradient, energy
```

```python
import functools
import jax
import jax.numpy as jnp
from jax import lax
from jax.experimental import pallas as pl
from jax.experimental.pallas import tpu as pltpu
from jax.sharding import PartitionSpec as P

step_size = 0.1
LANES = 128
CHUNKS = 4
MESH = pl.DeviceIdType.MESH
BF16 = jnp.bfloat16
F32 = jnp.float32


def iota(shape, dim):
    return lax.broadcasted_iota(jnp.int32, shape, dim)


def split(x):
    hi = x.astype(BF16)
    return hi, (x - hi.astype(F32)).astype(BF16)


def nt_dot(a, b):
    return lax.dot_general(a, b, (((1,), (1,)), ((), ())), preferred_element_type=F32)


def kernel(
    n, nf, chains, quarter,
    obs_hbm, lab_ref, grp_ref, pos_ref, mom_ref, grad_ref, par_ref,
    newpos_ref, newmom_ref, newgrad_ref, energy_ref,
    obs, perm, wsrc, wall, half_ref, lhs, mine, pair_send, pair_recv,
    far_send, far_recv, res_own, res_recv, nll_ref, dmat, gsend, grecv, esend, erecv,
    obs_sem, w_ssem, w_rsem, p_ssem, p_rsem, f_ssem, f_rsem, r_ssem, r_rsem,
    g_ssem, g_rsem, e_ssem, e_rsem,
):
    me = lax.axis_index("dp")
    feat = lax.axis_index("feat")
    tiles = lab_ref.shape[0]
    own, width = pos_ref.shape
    pack = LANES // quarter
    quads = tiles // pack
    qrows = pack * chains
    half_quads = quads // 2
    chunk_quads = half_quads // CHUNKS
    chunk_tiles = chunk_quads * pack
    crows = chunk_quads * qrows
    groups = n * own
    bit = feat % 2
    near = feat + 1 - 2 * bit
    far = (feat + nf // 2) % nf

    fetch = pltpu.make_async_copy(obs_hbm, obs, obs_sem)
    fetch.start()
    barrier = pltpu.get_barrier_semaphore()

    def greet(i, carry):
        pl.semaphore_signal(barrier, inc=1, device_id={"dp": (me + i) % n}, device_id_type=MESH)
        return carry

    lax.fori_loop(1, n, greet, 0)
    for i in range(1, nf):
        pl.semaphore_signal(barrier, inc=1, device_id={"feat": (feat + i) % nf}, device_id_type=MESH)

    r, c = iota((width, width), 0), iota((width, width), 1)
    perm[...] = jnp.where(
        (r % chains == c // quarter) & (r // chains == c % quarter), 1.0, 0.0
    ).astype(BF16)
    half = mom_ref[...] - 0.5 * step_size * grad_ref[...]
    half_ref[...] = half
    moved = pos_ref[...] + step_size * par_ref[2:3, :] * half
    newpos_ref[...] = moved
    coeff = jnp.dot(moved.astype(BF16), perm[...], preferred_element_type=F32).astype(BF16)
    wsrc[...] = coeff
    own_rows = pl.ds(pl.multiple_of(me * own, own), own)
    wall[own_rows, :] = coeff
    pl.semaphore_wait(barrier, n - 1 + nf - 1)

    def w_copy(i):
        to = (me + i) % n
        return pltpu.make_async_remote_copy(
            src_ref=wsrc, dst_ref=wall.at[own_rows], send_sem=w_ssem.at[i],
            recv_sem=w_rsem.at[i], device_id={"dp": to}, device_id_type=MESH,
        )

    def start_w(i, carry):
        w_copy(i).start()
        return carry

    lax.fori_loop(1, n, start_w, 0)
    seg_groups = min(groups, LANES)
    hot = (iota((groups, tiles), 0) == grp_ref[...]).astype(F32).astype(BF16)

    def wait_w(i, carry):
        w_copy(i).wait()
        return carry

    lax.fori_loop(1, n, wait_w, 0)
    picked = lax.dot_general(
        hot, wall[...], (((0,), (0,)), ((), ())), preferred_element_type=F32
    )
    row_t, lane_t = iota((tiles, LANES), 0), iota((tiles, LANES), 1)
    place = row_t % pack
    keep = lane_t // quarter == place
    for m in range(width // LANES):
        x = picked[:, m * LANES:(m + 1) * LANES]
        turned = [x] + [pltpu.roll(x, s * quarter, 1) for s in range(1, pack)]
        for j in range(pack):
            y = turned[0]
            for s in range(1, pack):
                y = jnp.where((place + pack - j) % pack == s, turned[s], y)
            lhs[pl.ds(m * pack + j, tiles, stride=chains), :] = jnp.where(keep, y, 0.0)
    fetch.wait()

    def logits(first_quad, dst, base):
        for i in range(chunk_quads):
            q = first_quad + i
            a = lhs[pl.ds(pl.multiple_of(q * qrows, qrows), qrows), :].astype(BF16)
            dst[pl.ds(pl.multiple_of(base + i * qrows, qrows), qrows), :] = jnp.dot(
                a, obs[q], preferred_element_type=F32
            )

    def rows(k):
        return pl.ds(pl.multiple_of(k * crows, crows), crows)

    def pair_copy(k):
        return pltpu.make_async_remote_copy(
            src_ref=pair_send.at[rows(k)], dst_ref=pair_recv.at[rows(k)],
            send_sem=p_ssem.at[k], recv_sem=p_rsem.at[k],
            device_id={"feat": near}, device_id_type=MESH,
        )

    def far_copy(k):
        return pltpu.make_async_remote_copy(
            src_ref=far_send.at[rows(k)], dst_ref=far_recv.at[rows(k)],
            send_sem=f_ssem.at[k], recv_sem=f_rsem.at[k],
            device_id={"feat": far}, device_id_type=MESH,
        )

    def res_copy(k):
        return pltpu.make_async_remote_copy(
            src_ref=res_own.at[rows(k)], dst_ref=res_recv.at[rows(k)],
            send_sem=r_ssem.at[k], recv_sem=r_rsem.at[k],
            device_id={"feat": near}, device_id_type=MESH,
        )

    def stage_a(k, carry):
        logits((1 - bit) * half_quads + k * chunk_quads, pair_send, k * crows)
        pair_copy(k).start()
        logits(bit * half_quads + k * chunk_quads, mine, k * crows)
        return carry

    lax.fori_loop(0, CHUNKS, stage_a, 0)

    def stage_b(k, carry):
        pair_copy(k).wait()
        total = mine[rows(k), :] + pair_recv[rows(k), :]
        mine[rows(k), :] = total
        far_send[rows(k), :] = total.astype(BF16)
        far_copy(k).start()
        return carry

    lax.fori_loop(0, CHUNKS, stage_b, 0)

    nll_ref[...] = jnp.zeros_like(nll_ref)
    diag = iota((qrows, LANES), 0) // chains == iota((qrows, LANES), 1) // quarter

    def grads(first_quad, src, k):
        for i in range(chunk_quads):
            q = first_quad + i
            a = src[pl.ds(pl.multiple_of(k * crows + i * qrows, qrows), qrows), :]
            g = jnp.where(diag, nt_dot(a, obs[q]), 0.0)
            for j in range(pack):
                dmat[pl.ds(q * pack + j, chains, stride=tiles), :] = g[j * chains:(j + 1) * chains]

    def stage_c(k, carry):
        far_copy(k).wait()
        z = mine[rows(k), :] + far_recv[rows(k), :].astype(F32)
        first = pl.multiple_of((bit * half_quads + k * chunk_quads) * pack, chunk_tiles)
        lab = lab_ref[pl.ds(first, chunk_tiles), :]
        lab = jnp.broadcast_to(lab[:, None, :], (chunk_tiles, chains, LANES)).reshape(crows, LANES)
        live = lab >= 0.0
        e = jnp.exp(-jnp.abs(z))
        inv = 1.0 / (1.0 + e)
        sig = jnp.where(z >= 0.0, inv, e * inv)
        res_own[rows(k), :] = jnp.where(live, sig - lab, 0.0).astype(BF16)
        res_copy(k).start()
        v = jnp.where(live, jnp.maximum(z, 0.0) + jnp.log1p(e) - lab * z, 0.0)
        s = jnp.sum(v, axis=1, keepdims=True) * (2.0 / nf)
        at = iota((crows, LANES), 0) % chains == iota((crows, LANES), 1)
        s = jnp.where(at, s, 0.0).reshape(chunk_tiles, chains, LANES)
        nll_ref[pl.ds(first, chunk_tiles), :] = jnp.sum(s, axis=1)
        grads(bit * half_quads + k * chunk_quads, res_own, k)
        return carry

    lax.fori_loop(0, CHUNKS, stage_c, 0)

    def stage_d(k, carry):
        res_copy(k).wait()
        grads((1 - bit) * half_quads + k * chunk_quads, res_recv, k)
        return carry

    lax.fori_loop(0, CHUNKS, stage_d, 0)

    lane_g = iota((seg_groups, LANES), 1) // quarter

    def segment(gc, carry):
        base = gc * seg_groups
        out = pl.ds(pl.multiple_of(base, seg_groups), seg_groups)
        oh = (iota((seg_groups, tiles), 0) + base == grp_ref[...]).astype(F32).astype(BF16)
        oh = jnp.concatenate([oh, oh], axis=1)

        def stacked(d):
            return jnp.concatenate(split(d), axis=0)

        for m in range(width // LANES):
            packed = None
            for j in range(0, pack, 2):
                at = (m * pack + j) * tiles
                rhs = jnp.concatenate(
                    [stacked(dmat[at:at + tiles]), stacked(dmat[at + tiles:at + 2 * tiles])], axis=1
                )
                both = jnp.dot(oh, rhs, preferred_element_type=F32)
                for h in range(2):
                    s = both[:, h * LANES:(h + 1) * LANES]
                    shift = LANES // 2
                    while shift >= quarter:
                        s = s + pltpu.roll(s, shift, 1)
                        shift //= 2
                    packed = s if packed is None else jnp.where(lane_g == j + h, s, packed)
            gsend[out, m * LANES:(m + 1) * LANES] = packed.astype(BF16)
        hi, lo = split(jnp.dot(oh, stacked(nll_ref[...]), preferred_element_type=F32))
        gsend[out, width:width + LANES] = (
            hi.astype(F32) + pltpu.roll(lo.astype(F32), chains, 1)
        ).astype(BF16)
        return carry

    lax.fori_loop(0, groups // seg_groups, segment, 0)

    def g_copy(i):
        to = (me + i) % n
        return pltpu.make_async_remote_copy(
            src_ref=gsend.at[pl.ds(pl.multiple_of(to * own, own), own)],
            dst_ref=grecv.at[me], send_sem=g_ssem.at[i], recv_sem=g_rsem.at[i],
            device_id={"dp": to}, device_id_type=MESH,
        )

    def start_g(i, carry):
        g_copy(i).start()
        return carry

    lax.fori_loop(1, n, start_g, 0)
    grecv[me] = gsend[own_rows, :]

    def wait_g(i, carry):
        g_copy(i).wait()
        return carry

    lax.fori_loop(1, n, wait_g, 0)

    def add_g(i, total):
        return total + grecv[i].astype(F32)

    total = lax.fori_loop(0, n, add_g, jnp.zeros((own, width + LANES), F32))
    parts = jnp.concatenate(split(total[:, :width]), axis=0)
    natural = nt_dot(parts, perm[...])
    lik = natural[:own] + natural[own:]
    mean, prec, mass = par_ref[0:1, :], par_ref[1:2, :], par_ref[2:3, :]
    offset = newpos_ref[...] - mean
    new_gradient = lik + prec * offset
    new_momentum = half_ref[...] - 0.5 * step_size * new_gradient
    newgrad_ref[...] = new_gradient
    newmom_ref[...] = new_momentum
    quad = 0.5 * (prec * offset * offset + mass * new_momentum * new_momentum)
    q = quad[:, :LANES]
    for m in range(1, width // LANES):
        q = q + quad[:, m * LANES:(m + 1) * LANES]
    shift = LANES // 2
    while shift >= chains:
        q = q + pltpu.roll(q, shift, 1)
        shift //= 2
    loss = total[:, width:]
    loss = loss + pltpu.roll(loss, LANES - chains, 1)
    esend[...] = q + loss

    def e_copy(i):
        return pltpu.make_async_remote_copy(
            src_ref=esend, dst_ref=erecv.at[feat], send_sem=e_ssem.at[i],
            recv_sem=e_rsem.at[i], device_id={"feat": (feat + i) % nf}, device_id_type=MESH,
        )

    for i in range(1, nf):
        e_copy(i).start()
    erecv[feat] = esend[...]
    for i in range(1, nf):
        e_copy(i).wait()
    e = erecv[0]
    for i in range(1, nf):
        e = e + erecv[i]
    energy_ref[...] = e[:, :chains]


def body(observations, labels, tile_live, tile_group, position, momentum, gradient, prior_mean, prior_prec, inv_mass):
    n, nf = lax.axis_size("dp"), lax.axis_size("feat")
    tiles, quarter, row_count = observations.shape
    own, width = position.shape
    chains = width // quarter
    pack = LANES // quarter
    alive = jnp.arange(row_count, dtype=jnp.int32)[None, :] < tile_live[:, None]
    marked = jnp.where(alive, labels, -1).astype(F32)
    par = jnp.stack([prior_mean, jnp.repeat(prior_prec, chains), jnp.repeat(inv_mass, chains)])
    half_rows = tiles * chains // 2
    vmem = pl.BlockSpec(memory_space=pltpu.VMEM)
    dma = pltpu.SemaphoreType.DMA
    block = jax.ShapeDtypeStruct((own, width), F32)
    return tuple(pl.pallas_call(
        functools.partial(kernel, n, nf, chains, quarter),
        out_shape=(block, block, block, jax.ShapeDtypeStruct((own, chains), F32)),
        in_specs=[pl.BlockSpec(memory_space=pl.ANY)] + [vmem] * 6,
        out_specs=(vmem,) * 4,
        scratch_shapes=[
            pltpu.VMEM((tiles // pack, LANES, row_count), BF16),
            pltpu.VMEM((width, width), BF16),
            pltpu.VMEM((own, width), BF16),
            pltpu.VMEM((n * own, width), BF16),
            pltpu.VMEM((own, width), F32),
            pltpu.VMEM((tiles * chains, LANES), F32),
            pltpu.VMEM((half_rows, row_count), F32),
            pltpu.VMEM((half_rows, row_count), F32),
            pltpu.VMEM((half_rows, row_count), F32),
            pltpu.VMEM((half_rows, row_count), BF16),
            pltpu.VMEM((half_rows, row_count), BF16),
            pltpu.VMEM((half_rows, row_count), BF16),
            pltpu.VMEM((half_rows, row_count), BF16),
            pltpu.VMEM((tiles, LANES), F32),
            pltpu.VMEM((chains * tiles, LANES), F32),
            pltpu.VMEM((n * own, width + LANES), BF16),
            pltpu.VMEM((n, own, width + LANES), BF16),
            pltpu.VMEM((own, LANES), F32),
            pltpu.VMEM((nf, own, LANES), F32),
            dma,
            dma((n,)), dma((n,)),
            dma((CHUNKS,)), dma((CHUNKS,)),
            dma((CHUNKS,)), dma((CHUNKS,)),
            dma((CHUNKS,)), dma((CHUNKS,)),
            dma((n,)), dma((n,)),
            dma((nf,)), dma((nf,)),
        ],
        compiler_params=pltpu.CompilerParams(collective_id=0, has_side_effects=True),
    )(
        observations.reshape(tiles // pack, LANES, row_count),
        marked,
        tile_group.reshape(1, tiles),
        position, momentum, gradient, par,
    ))


def solution(mesh):
    placed = (
        P("dp", "feat", None),
        P("dp", None),
        P("dp"),
        P("dp"),
        P("dp", "feat"),
        P("dp", "feat"),
        P("dp", "feat"),
        P("feat"),
        P("feat"),
        P("feat"),
    )
    return jax.shard_map(
        body,
        mesh=mesh,
        in_specs=placed,
        out_specs=(P("dp", "feat"), P("dp", "feat"), P("dp", "feat"), P("dp", None)),
        check_vma=False,
    )
```

```python
import functools
import jax
import jax.numpy as jnp
from jax import lax
from jax.experimental import pallas as pl
from jax.experimental.pallas import tpu as pltpu
from jax.sharding import PartitionSpec as P

step_size = 0.1
LANES = 128
CHUNKS = 8
MESH = pl.DeviceIdType.MESH
BF16 = jnp.bfloat16
F32 = jnp.float32


def iota(shape, dim):
    return lax.broadcasted_iota(jnp.int32, shape, dim)


def split(x):
    hi = x.astype(BF16)
    return hi, (x - hi.astype(F32)).astype(BF16)


def nt_dot(a, b):
    return lax.dot_general(a, b, (((1,), (1,)), ((), ())), preferred_element_type=F32)


def kernel(
    n, nf, chains, quarter,
    obs_hbm, lab_hbm, live_hbm, grp_hbm, pos_hbm, mom_hbm, grad_hbm, mean_hbm, prec_hbm, mass_hbm,
    newpos_out, newmom_out, newgrad_out, energy_out,
    lab_in, live_ref, grp_ref, pos_ref, mom_ref, grad_ref, mean_ref, pair_ref,
    lab_ref, par_ref, newpos_ref, newmom_ref, newgrad_ref, energy_ref, obs, perm, wsrc, wall, half_ref, lhs, mine, pair_send, pair_recv,
    far_send, far_recv, res_own, res_recv, nll_ref, dmat, gsend0, gsend1, grecv0, grecv1, esend, erecv,
    in_sem, out_sem, w_ssem, w_rsem, p_ssem, p_rsem, f_ssem, f_rsem, r_ssem, r_rsem,
    g_ssem, g_rsem, e_ssem, e_rsem,
):
    me = lax.axis_index("dp")
    feat = lax.axis_index("feat")
    tiles = lab_ref.shape[0]
    own, width = pos_ref.shape
    pack = LANES // quarter
    quads = tiles // pack
    qrows = pack * chains
    half_quads = quads // 2
    chunk_quads = half_quads // CHUNKS
    chunk_tiles = chunk_quads * pack
    crows = chunk_quads * qrows
    groups = n * own
    bit = feat % 2
    near = feat + 1 - 2 * bit
    far = (feat + nf // 2) % nf

    barrier = pltpu.get_barrier_semaphore()

    def greet(i, carry):
        pl.semaphore_signal(barrier, inc=1, device_id={"dp": (me + i) % n}, device_id_type=MESH)
        return carry

    lax.fori_loop(1, n, greet, 0)
    for i in range(1, nf):
        pl.semaphore_signal(barrier, inc=1, device_id={"feat": (feat + i) % nf}, device_id_type=MESH)

    sources = [
        (pos_hbm, pos_ref), (mom_hbm, mom_ref), (grad_hbm, grad_ref), (mean_hbm, mean_ref),
        (prec_hbm, pair_ref.at[0:1]), (mass_hbm, pair_ref.at[1:2]), (grp_hbm, grp_ref),
        (live_hbm, live_ref), (lab_hbm, lab_in), (obs_hbm, obs),
    ]
    fetches = [pltpu.make_async_copy(a, b, in_sem.at[i]) for i, (a, b) in enumerate(sources)]
    for f in fetches:
        f.start()
    spread = (iota((quarter, width), 0) == iota((quarter, width), 1) // chains).astype(F32)
    r, c = iota((width, width), 0), iota((width, width), 1)
    perm[...] = jnp.where(
        (r % chains == c // quarter) & (r // chains == c % quarter), 1.0, 0.0
    ).astype(BF16)
    for f in fetches[:-1]:
        f.wait()
    par_ref[...] = jnp.dot(
        pair_ref[...], spread, precision=lax.Precision.HIGHEST, preferred_element_type=F32
    )
    half = mom_ref[...] - 0.5 * step_size * grad_ref[...]
    half_ref[...] = half
    moved = pos_ref[...] + step_size * par_ref[1:2, :] * half
    newpos_ref[...] = moved
    out_pos = pltpu.make_async_copy(newpos_ref, newpos_out, out_sem.at[0])
    out_pos.start()
    coeff = jnp.dot(moved.astype(BF16), perm[...], preferred_element_type=F32).astype(BF16)
    wsrc[...] = coeff
    own_rows = pl.ds(pl.multiple_of(me * own, own), own)
    wall[own_rows, :] = coeff
    square = iota((tiles, tiles), 0) == iota((tiles, tiles), 1)
    live_col = jnp.sum(jnp.where(square, live_ref[...].astype(F32), 0.0), axis=1, keepdims=True)
    lab_ref[...] = jnp.where(
        iota(lab_ref.shape, 1).astype(F32) < live_col, lab_in[...].astype(F32), -1.0
    )
    nll_ref[...] = jnp.zeros_like(nll_ref)
    pl.semaphore_wait(barrier, n - 1 + nf - 1)

    def w_copy(i):
        to = (me + i) % n
        return pltpu.make_async_remote_copy(
            src_ref=wsrc, dst_ref=wall.at[own_rows], send_sem=w_ssem.at[i],
            recv_sem=w_rsem.at[i], device_id={"dp": to}, device_id_type=MESH,
        )

    def start_w(i, carry):
        w_copy(i).start()
        return carry

    lax.fori_loop(1, n, start_w, 0)
    seg_groups = min(groups, LANES)
    hot = (iota((groups, tiles), 0) == grp_ref[...]).astype(F32).astype(BF16)

    def wait_w(i, carry):
        w_copy(i).wait()
        return carry

    lax.fori_loop(1, n, wait_w, 0)
    picked = lax.dot_general(
        hot, wall[...], (((0,), (0,)), ((), ())), preferred_element_type=F32
    )
    row_t, lane_t = iota((tiles, LANES), 0), iota((tiles, LANES), 1)
    place = row_t % pack
    keep = lane_t // quarter == place
    for m in range(width // LANES):
        x = picked[:, m * LANES:(m + 1) * LANES]
        turned = [x] + [pltpu.roll(x, s * quarter, 1) for s in range(1, pack)]
        for j in range(pack):
            y = turned[0]
            for s in range(1, pack):
                y = jnp.where((place + pack - j) % pack == s, turned[s], y)
            lhs[pl.ds(m * pack + j, tiles, stride=chains), :] = jnp.where(keep, y, 0.0)
    fetches[-1].wait()

    def logits(first_quad, dst, base):
        for i in range(chunk_quads):
            q = first_quad + i
            a = lhs[pl.ds(pl.multiple_of(q * qrows, qrows), qrows), :].astype(BF16)
            dst[pl.ds(pl.multiple_of(base + i * qrows, qrows), qrows), :] = jnp.dot(
                a, obs[q], preferred_element_type=F32
            )

    def rows(k):
        return pl.ds(pl.multiple_of(k * crows, crows), crows)

    def pair_copy(k):
        return pltpu.make_async_remote_copy(
            src_ref=pair_send.at[rows(k)], dst_ref=pair_recv.at[rows(k)],
            send_sem=p_ssem.at[k], recv_sem=p_rsem.at[k],
            device_id={"feat": near}, device_id_type=MESH,
        )

    def far_copy(k):
        return pltpu.make_async_remote_copy(
            src_ref=far_send.at[rows(k)], dst_ref=far_recv.at[rows(k)],
            send_sem=f_ssem.at[k], recv_sem=f_rsem.at[k],
            device_id={"feat": far}, device_id_type=MESH,
        )

    def res_copy(k):
        return pltpu.make_async_remote_copy(
            src_ref=res_own.at[rows(k)], dst_ref=res_recv.at[rows(k)],
            send_sem=r_ssem.at[k], recv_sem=r_rsem.at[k],
            device_id={"feat": near}, device_id_type=MESH,
        )

    def stage_a(k, carry):
        logits((1 - bit) * half_quads + k * chunk_quads, pair_send, k * crows)
        pair_copy(k).start()
        logits(bit * half_quads + k * chunk_quads, mine, k * crows)
        return carry


    def stage_b(k, carry):
        pair_copy(k).wait()
        total = mine[rows(k), :] + pair_recv[rows(k), :]
        mine[rows(k), :] = total
        far_send[rows(k), :] = total.astype(BF16)
        far_copy(k).start()
        return carry

    def stage_ab(k, carry):
        stage_a(k, 0)
        stage_b(k - 1, 0)
        return carry

    stage_a(0, 0)
    lax.fori_loop(1, CHUNKS, stage_ab, 0)
    stage_b(CHUNKS - 1, 0)

    diag = iota((qrows, LANES), 0) // chains == iota((qrows, LANES), 1) // quarter

    def grads(first_quad, src, k):
        for i in range(chunk_quads):
            q = first_quad + i
            a = src[pl.ds(pl.multiple_of(k * crows + i * qrows, qrows), qrows), :]
            g = jnp.where(diag, nt_dot(a, obs[q]), 0.0)
            for j in range(pack):
                dmat[pl.ds(q * pack + j, chains, stride=tiles), :] = g[j * chains:(j + 1) * chains]

    def stage_c(k, carry):
        far_copy(k).wait()
        z = mine[rows(k), :] + far_recv[rows(k), :].astype(F32)
        first = pl.multiple_of((bit * half_quads + k * chunk_quads) * pack, chunk_tiles)
        lab = lab_ref[pl.ds(first, chunk_tiles), :]
        lab = jnp.broadcast_to(lab[:, None, :], (chunk_tiles, chains, LANES)).reshape(crows, LANES)
        live = lab >= 0.0
        e = jnp.exp(-jnp.abs(z))
        inv = 1.0 / (1.0 + e)
        sig = jnp.where(z >= 0.0, inv, e * inv)
        res_own[rows(k), :] = jnp.where(live, sig - lab, 0.0).astype(BF16)
        res_copy(k).start()
        v = jnp.where(live, jnp.maximum(z, 0.0) + jnp.log1p(e) - lab * z, 0.0)
        s = jnp.sum(v, axis=1, keepdims=True) * (2.0 / nf)
        at = iota((crows, LANES), 0) % chains == iota((crows, LANES), 1)
        s = jnp.where(at, s, 0.0).reshape(chunk_tiles, chains, LANES)
        nll_ref[pl.ds(first, chunk_tiles), :] = jnp.sum(s, axis=1)
        grads(bit * half_quads + k * chunk_quads, res_own, k)
        return carry

    lax.fori_loop(0, CHUNKS, stage_c, 0)

    def stage_d(k, carry):
        res_copy(k).wait()
        grads((1 - bit) * half_quads + k * chunk_quads, res_recv, k)
        return carry

    lax.fori_loop(0, CHUNKS, stage_d, 0)

    lane_g = iota((seg_groups, LANES), 1) // quarter
    count = width // LANES
    cut = count // 2
    sums = ((gsend0, grecv0, range(cut), True), (gsend1, grecv1, range(cut, count), False))

    def stacked(d):
        return jnp.concatenate(split(d), axis=0)

    def segment(gc, part):
        gsend, _, blocks, with_nll = sums[part]
        base = gc * seg_groups
        out = pl.ds(pl.multiple_of(base, seg_groups), seg_groups)
        oh = (iota((seg_groups, tiles), 0) + base == grp_ref[...]).astype(F32).astype(BF16)
        oh = jnp.concatenate([oh, oh], axis=1)
        for b, m in enumerate(blocks):
            packed = None
            for j in range(0, pack, 2):
                at = (m * pack + j) * tiles
                rhs = jnp.concatenate(
                    [stacked(dmat[at:at + tiles]), stacked(dmat[at + tiles:at + 2 * tiles])], axis=1
                )
                both = jnp.dot(oh, rhs, preferred_element_type=F32)
                for h in range(2):
                    s = both[:, h * LANES:(h + 1) * LANES]
                    shift = LANES // 2
                    while shift >= quarter:
                        s = s + pltpu.roll(s, shift, 1)
                        shift //= 2
                    packed = s if packed is None else jnp.where(lane_g == j + h, s, packed)
            gsend[out, b * LANES:(b + 1) * LANES] = packed.astype(BF16)
        if with_nll:
            hi, lo = split(jnp.dot(oh, stacked(nll_ref[...]), preferred_element_type=F32))
            gsend[out, len(blocks) * LANES:] = (
                hi.astype(F32) + pltpu.roll(lo.astype(F32), chains, 1)
            ).astype(BF16)

    def g_copy(part, i):
        to = (me + i) % n
        return pltpu.make_async_remote_copy(
            src_ref=sums[part][0].at[pl.ds(pl.multiple_of(to * own, own), own)],
            dst_ref=sums[part][1].at[me], send_sem=g_ssem.at[part, i], recv_sem=g_rsem.at[part, i],
            device_id={"dp": to}, device_id_type=MESH,
        )

    for part in range(2):
        def run(gc, carry, part=part):
            segment(gc, part)
            return carry

        def start_g(i, carry, part=part):
            g_copy(part, i).start()
            return carry

        lax.fori_loop(0, groups // seg_groups, run, 0)
        lax.fori_loop(1, n, start_g, 0)
        sums[part][1][me] = sums[part][0][own_rows, :]

    def wait_g(i, carry):
        g_copy(0, i).wait()
        g_copy(1, i).wait()
        return carry

    lax.fori_loop(1, n, wait_g, 0)

    def add_g(i, total):
        return total[0] + grecv0[i].astype(F32), total[1] + grecv1[i].astype(F32)

    first, second = lax.fori_loop(0, n, add_g, (
        jnp.zeros((own, (cut + 1) * LANES), F32), jnp.zeros((own, (count - cut) * LANES), F32)
    ))
    lik_packed = jnp.concatenate([first[:, :cut * LANES], second], axis=1)
    parts = jnp.concatenate(split(lik_packed), axis=0)
    natural = nt_dot(parts, perm[...])
    lik = natural[:own] + natural[own:]
    mean, prec, mass = mean_ref[...], par_ref[0:1, :], par_ref[1:2, :]
    offset = newpos_ref[...] - mean
    new_gradient = lik + prec * offset
    new_momentum = half_ref[...] - 0.5 * step_size * new_gradient
    newgrad_ref[...] = new_gradient
    newmom_ref[...] = new_momentum
    out_grad = pltpu.make_async_copy(newgrad_ref, newgrad_out, out_sem.at[1])
    out_mom = pltpu.make_async_copy(newmom_ref, newmom_out, out_sem.at[2])
    out_grad.start()
    out_mom.start()
    quad = 0.5 * (prec * offset * offset + mass * new_momentum * new_momentum)
    q = quad[:, :LANES]
    for m in range(1, width // LANES):
        q = q + quad[:, m * LANES:(m + 1) * LANES]
    shift = LANES // 2
    while shift >= chains:
        q = q + pltpu.roll(q, shift, 1)
        shift //= 2
    loss = first[:, cut * LANES:]
    loss = loss + pltpu.roll(loss, LANES - chains, 1)
    esend[...] = q + loss

    def e_copy(i):
        return pltpu.make_async_remote_copy(
            src_ref=esend, dst_ref=erecv.at[feat], send_sem=e_ssem.at[i],
            recv_sem=e_rsem.at[i], device_id={"feat": (feat + i) % nf}, device_id_type=MESH,
        )

    for i in range(1, nf):
        e_copy(i).start()
    erecv[feat] = esend[...]
    for i in range(1, nf):
        e_copy(i).wait()
    e = erecv[0]
    for i in range(1, nf):
        e = e + erecv[i]
    energy_ref[...] = e[:, :chains]
    out_energy = pltpu.make_async_copy(energy_ref, energy_out, out_sem.at[3])
    out_energy.start()
    for f in (out_pos, out_grad, out_mom, out_energy):
        f.wait()


def finish(*refs):
    for a, b in zip(refs[:4], refs[4:]):
        b[...] = a[...]


def body(observations, labels, tile_live, tile_group, position, momentum, gradient, prior_mean, prior_prec, inv_mass):
    n, nf = lax.axis_size("dp"), lax.axis_size("feat")
    tiles, quarter, row_count = observations.shape
    own, width = position.shape
    chains = width // quarter
    pack = LANES // quarter
    half_rows = tiles * chains // 2
    anywhere = pl.BlockSpec(memory_space=pl.ANY)
    cut = width // LANES // 2 * LANES
    dma = pltpu.SemaphoreType.DMA
    block = jax.ShapeDtypeStruct((own, width), F32)
    results = pl.pallas_call(
        functools.partial(kernel, n, nf, chains, quarter),
        out_shape=(block, block, block, jax.ShapeDtypeStruct((own, chains), F32)),
        in_specs=[anywhere] * 10,
        out_specs=(anywhere,) * 4,
        scratch_shapes=[
            pltpu.VMEM((tiles, row_count), jnp.int32),
            pltpu.VMEM((1, tiles), jnp.int32),
            pltpu.VMEM((1, tiles), jnp.int32),
            pltpu.VMEM((own, width), F32),
            pltpu.VMEM((own, width), F32),
            pltpu.VMEM((own, width), F32),
            pltpu.VMEM((1, width), F32),
            pltpu.VMEM((2, quarter), F32),
            pltpu.VMEM((tiles, row_count), F32),
            pltpu.VMEM((2, width), F32),
            pltpu.VMEM((own, width), F32),
            pltpu.VMEM((own, width), F32),
            pltpu.VMEM((own, width), F32),
            pltpu.VMEM((own, chains), F32),
            pltpu.VMEM((tiles // pack, LANES, row_count), BF16),
            pltpu.VMEM((width, width), BF16),
            pltpu.VMEM((own, width), BF16),
            pltpu.VMEM((n * own, width), BF16),
            pltpu.VMEM((own, width), F32),
            pltpu.VMEM((tiles * chains, LANES), F32),
            pltpu.VMEM((half_rows, row_count), F32),
            pltpu.VMEM((half_rows, row_count), F32),
            pltpu.VMEM((half_rows, row_count), F32),
            pltpu.VMEM((half_rows, row_count), BF16),
            pltpu.VMEM((half_rows, row_count), BF16),
            pltpu.VMEM((half_rows, row_count), BF16),
            pltpu.VMEM((half_rows, row_count), BF16),
            pltpu.VMEM((tiles, LANES), F32),
            pltpu.VMEM((chains * tiles, LANES), F32),
            pltpu.VMEM((n * own, cut + LANES), BF16),
            pltpu.VMEM((n * own, width - cut), BF16),
            pltpu.VMEM((n, own, cut + LANES), BF16),
            pltpu.VMEM((n, own, width - cut), BF16),
            pltpu.VMEM((own, LANES), F32),
            pltpu.VMEM((nf, own, LANES), F32),
            dma((10,)), dma((4,)),
            dma((n,)), dma((n,)),
            dma((CHUNKS,)), dma((CHUNKS,)),
            dma((CHUNKS,)), dma((CHUNKS,)),
            dma((CHUNKS,)), dma((CHUNKS,)),
            dma((2, n)), dma((2, n)),
            dma((nf,)), dma((nf,)),
        ],
        compiler_params=pltpu.CompilerParams(collective_id=0, has_side_effects=True),
    )(
        observations.reshape(tiles // pack, LANES, row_count),
        labels, tile_live.reshape(1, tiles), tile_group.reshape(1, tiles),
        position, momentum, gradient,
        prior_mean.reshape(1, width), prior_prec.reshape(1, quarter), inv_mass.reshape(1, quarter),
    )
    return tuple(pl.pallas_call(
        finish,
        out_shape=tuple(jax.ShapeDtypeStruct(x.shape, x.dtype) for x in results),
        in_specs=[pl.BlockSpec(memory_space=pltpu.VMEM)] * 4,
        out_specs=(pl.BlockSpec(memory_space=pltpu.VMEM),) * 4,
    )(*results))


def solution(mesh):
    placed = (
        P("dp", "feat", None),
        P("dp", None),
        P("dp"),
        P("dp"),
        P("dp", "feat"),
        P("dp", "feat"),
        P("dp", "feat"),
        P("feat"),
        P("feat"),
        P("feat"),
    )
    return jax.shard_map(
        body,
        mesh=mesh,
        in_specs=placed,
        out_specs=(P("dp", "feat"), P("dp", "feat"), P("dp", "feat"), P("dp", None)),
        check_vma=False,
    )
```
